256 devices in a mesh: dp: 16 (over x, z_lo, core), tensor: 16 (over z_hi, y).
Axes of the slice: x: 4, y: 4, z: 8 (z_hi: 4, z_lo: 2; z = z_hi * 2 + z_lo), core: 2. Of those that a mesh axis runs over, the one named last changes fastest.
Arguments:
- out_grad: bfloat16 [2, 1280, 4096], P(None, 'dp', 'tensor'), may hold values from -0.15625 to 0.15625
- layer_input: bfloat16 [2, 1280, 4096], P(None, 'dp', 'tensor'), may hold values from -8 to 8
- w_down: bfloat16 [16384, 4096], P('tensor'), may hold values from -0.046875 to 0.046875
- silu_gate: bfloat16 [2, 1280, 16384], P(None, 'dp', 'tensor'), may hold values from -6 to 6
- up_proj: bfloat16 [2, 1280, 16384], P(None, 'dp', 'tensor'), may hold values from -6 to 6
- slope_codes: int32 [2, 128, 16384], P(None, 'dp', 'tensor'), may hold values from 0 to 1073741823
Outputs:
- grad_down: bfloat16 [16384, 4096], P('tensor', 'dp')
- grad_gate: bfloat16 [4096, 16384], P('dp', 'tensor')
- grad_up: bfloat16 [4096, 16384], P('dp', 'tensor')
The draws below stay inside these ranges and needn't reach their ends.
Inputs may be any that keep to these rules, and one draw needn't show every extreme that they name: `slope_codes`: every word holds ten independent 3-bit codes; all eight codes occur.
All inputs are finite; a program needn't handle non-finite values.
Results may differ from the reference program's by a relative error of at most 0.018.
Values may be sent and summed in bfloat16 or wider, within the bound.
A program may use at most 128 MiB of HBM per device.

```python
import jax
import jax.numpy as jnp
from jax import lax

D = 4096
FF = 16384
MICRO = 2
TOK_MB = 80
TOKENS = 1280
N_DP = 16


def plant(values, key, smallest, top_value):
    longest = values.shape.index(max(values.shape))
    spots = []
    for shift in (0, 1):
        where = [jax.random.randint(jax.random.fold_in(key, axis), (), 0, length) for axis, length in enumerate(values.shape)]
        where[longest] = (where[longest] + shift) % values.shape[longest]
        spots.append(tuple(where))
    return values.at[spots[0]].set(smallest).at[spots[1]].set(top_value)


def spiked(drawn, stream_key, source, target, shards_of, factor):
    def block_of(axis_at):
        return (jnp.arange(drawn.shape[axis_at]) // (drawn.shape[axis_at] // shards_of)).reshape((-1,) + (1,) * (drawn.ndim - 1 - axis_at))

    near = jax.random.permutation(stream_key, shards_of)[block_of(target)]
    other_side = (block_of(target) + shards_of // 2) % shards_of
    return jnp.where((block_of(source) == near) | (block_of(source) == other_side), factor * drawn, drawn)


def levels(rng, extent, split, smallest, largest):
    gain = 1.0
    for axis_at, blocks in split:
        draws = jax.random.uniform(jax.random.fold_in(jax.random.fold_in(rng, 6), axis_at), (blocks,), jnp.float32, smallest / len(split), largest / len(split))
        gain = gain * jnp.repeat(jnp.exp(draws), extent[axis_at] // blocks).reshape((-1,) + (1,) * (len(extent) - 1 - axis_at))
    return gain


def normal_values(stream_key, shape, scale, limit, cuts=(), kind=jnp.bfloat16):
    level = levels(stream_key, shape, cuts, -0.22, 0.18) if cuts else 1.0
    array = jax.random.normal(stream_key, shape, jnp.float32) * scale * level
    return jnp.minimum(jnp.maximum(array, -limit), limit).astype(kind)


def heavy_noise(rng, shape, spread, reach, split, heavy, held_as=jnp.bfloat16):
    values = spread * jax.random.normal(rng, shape, jnp.float32)
    if split:
        values = values * levels(rng, shape, split, -0.22, 0.18)
    return jnp.clip(spiked(values, jax.random.fold_in(rng, 3), *heavy), -reach, reach).astype(held_as)


def setup_inputs(seed: int = 0) -> dict:
    streams_of = jax.random.split(jax.random.key(seed), 7)
    return {
        "out_grad": heavy_noise(streams_of[0], (MICRO, TOKENS, D), (1.0 / (MICRO * TOKENS) ** 0.5), 0.15625, ((1, 16), (2, 16)), (1, 2, 16, 2.0)),
        "layer_input": heavy_noise(streams_of[1], (MICRO, TOKENS, D), 1.0, 8.0, ((1, 16), (2, 16)), (1, 2, 16, 2.0)),
        "w_down": normal_values(streams_of[2], (FF, D), FF ** -0.5, 0.046875, ((0, 16),)),
        "silu_gate": normal_values(streams_of[3], (MICRO, TOKENS, FF), 1.0, 6.0, ((1, 16), (2, 16))),
        "up_proj": normal_values(streams_of[4], (MICRO, TOKENS, FF), 1.0, 6.0, ((1, 16), (2, 16))),
        "slope_codes": plant(jax.random.randint(streams_of[5], (MICRO, TOKENS // 10, FF), 0, 1073741824), jax.random.fold_in(streams_of[5], 1), 0, 1073741823).astype(jnp.int32),
    }


SLOPE_LEVELS = (-0.09, 0.06, 0.22, 0.41, 0.6, 0.79, 0.96, 1.08)


def decode_slopes(packed):
    shifts = 3 * jnp.arange(10, dtype=jnp.int32)
    pieces = jnp.bitwise_and(jnp.right_shift(packed[..., None, :], shifts[:, None]), 7)
    pieces = pieces.reshape(packed.shape[:-2] + (packed.shape[-2] * 10, packed.shape[-1]))
    result = jnp.full(pieces.shape, SLOPE_LEVELS[0], jnp.float32)
    for symbol in range(1, 8):
        result = jnp.where(pieces == symbol, jnp.float32(SLOPE_LEVELS[symbol]), result)
    return result


def rounded(values):
    return lax.optimization_barrier(values.astype(jnp.bfloat16)).astype(jnp.float32)


def by_group(values):
    columns = values.shape[-1]
    shaped = values.reshape(MICRO, N_DP, TOK_MB, columns).transpose(1, 0, 2, 3)
    return shaped.reshape(N_DP, MICRO * TOK_MB, columns)


def reference(out_grad, layer_input, w_down, silu_gate, up_proj, slope_codes):
    slopes = decode_slopes(slope_codes)
    hidden_grad = jnp.dot(out_grad.reshape(-1, D), w_down.T, preferred_element_type=jnp.float32)
    hidden_grad = hidden_grad.reshape(MICRO, -1, FF)
    gate_act = silu_gate.astype(jnp.float32)
    up_value = up_proj.astype(jnp.float32)
    up_grad = (hidden_grad * gate_act).astype(jnp.bfloat16)
    gate_grad = (hidden_grad * up_value * slopes).astype(jnp.bfloat16)
    hidden = (gate_act * up_value).astype(jnp.bfloat16)

    def add_group(totals, pieces):
        inputs, output_rows, hidden_rows, gate_rows, up_rows = pieces
        gate_part = jnp.dot(inputs.T, gate_rows, preferred_element_type=jnp.float32)
        up_part = jnp.dot(inputs.T, up_rows, preferred_element_type=jnp.float32)
        down_part = jnp.dot(hidden_rows.T, output_rows, preferred_element_type=jnp.float32)
        return (totals[0] + rounded(gate_part), totals[1] + rounded(up_part), totals[2] + rounded(down_part)), None

    start_totals = (jnp.zeros((D, FF), jnp.float32), jnp.zeros((D, FF), jnp.float32), jnp.zeros((FF, D), jnp.float32))
    totals, unused = lax.scan(add_group, start_totals, (by_group(layer_input), by_group(out_grad), by_group(hidden), by_group(gate_grad), by_group(up_grad)))
    return (totals[2].astype(jnp.bfloat16), totals[0].astype(jnp.bfloat16), totals[1].astype(jnp.bfloat16))
```

```python
import jax
import jax.numpy as jnp
from jax import lax
from jax.experimental import pallas as pl
from jax.experimental.pallas import tpu as pltpu
from jax.sharding import PartitionSpec as P

SLOPE_LEVELS = (-0.09, 0.06, 0.22, 0.41, 0.6, 0.79, 0.96, 1.08)
MESH = pl.DeviceIdType.MESH
ROWS = 160
HALF = 80
BLOCK = 256
HIDDEN = 1024
WIDTH = 4096
CHUNKS = 4
PART = HIDDEN // CHUNKS
WIDE = 2 * PART
N_COPIES = 128


def wrap(value):
    return lax.rem(value + 4, 4)


def kernel(
    dy_hbm, x_hbm, w_hbm, s_hbm, u_hbm, code_hbm,
    down_ref, gate_ref, up_ref,
    dyv, xv, wv, sv, uv, cv, rows, xt, dyt, hid, gu, h, slopes, xtt, dytt, psend, precv, pown,
    lsem, ssem, rsem, tsem,
):
    dp = lax.axis_index("dp")
    tensor = lax.axis_index("tensor")
    x, zl, c = dp // 4, lax.rem(dp // 2, 2), lax.rem(dp, 2)
    zh, y = tensor // 4, lax.rem(tensor, 4)
    y1, y0 = y // 2, lax.rem(y, 2)

    def device(x=x, zl=zl, c=c, zh=zh, y=y):
        return {"dp": x * 4 + zl * 2 + c, "tensor": zh * 4 + y}

    swap_x = device(zh, zl, y0, x, y1 * 2 + c)
    swap_d = {"dp": tensor, "tensor": dp}
    alone_x = jnp.logical_and(x == zh, c == y0)
    alone_d = dp == tensor
    ring = {
        "x+": device(x=wrap(x + 1)), "x-": device(x=wrap(x - 1)),
        "y+": device(y=wrap(y + 1)), "y-": device(y=wrap(y - 1)),
        "z+": device(zh=wrap(zh + 1)), "z-": device(zh=wrap(zh - 1)),
        "core": device(c=1 - c), "pair": device(zl=1 - zl),
    }

    barrier = pltpu.get_barrier_semaphore()
    for peer in ring.values():
        pl.semaphore_signal(barrier, inc=1, device_id=peer, device_id_type=MESH)

    @pl.when(jnp.logical_not(alone_x))
    def _():
        pl.semaphore_signal(barrier, inc=1, device_id=swap_x, device_id_type=MESH)

    @pl.when(jnp.logical_not(alone_d))
    def _():
        pl.semaphore_signal(barrier, inc=1, device_id=swap_d, device_id_type=MESH)

    local = [
        pltpu.make_async_copy(src, dst, lsem.at[i])
        for i, (src, dst) in enumerate(
            ((dy_hbm, dyv), (x_hbm, xv), (s_hbm, sv), (u_hbm, uv), (code_hbm, cv), (w_hbm, wv))
        )
    ]
    for copy in local:
        copy.start()

    sent = []

    def send(src, dst, peer):
        i = len(sent)
        copy = pltpu.make_async_remote_copy(
            src_ref=src, dst_ref=dst, send_sem=ssem.at[i], recv_sem=rsem.at[i], device_id=peer, device_id_type=MESH
        )
        copy.start()
        sent.append(copy)
        return copy

    def rows_at(buffer, row, start=0, size=ROWS):
        return buffer.at[pl.ds(pl.multiple_of(row * ROWS + start, 16), size)]

    def at_rows(zh, y, start=0, size=ROWS):
        return rows_at(rows, zh * 4 + y, start, size)

    def at_xt(zh, y, start=0, size=ROWS):
        return rows_at(xt, (y // 2) * 8 + zh * 2 + lax.rem(y, 2), start, size)

    def at_dyt(zh, y, start=0, size=ROWS):
        return rows_at(dyt, zh * 4 + y, start, size)

    class Gather:
        def __init__(self, at):
            self.at = at
            self.right, self.left, self.tops, self.bottoms = {}, {}, {}, {}
            self.origin = (zh, wrap(zh - 1), wrap(zh + 1), wrap(zh + 2))

        def along_y(self, b, first=None):
            block = self.at(self.origin[b], y)
            src = block if first is None else first
            self.right[b] = send(src, block, ring["y+"])
            self.left[b] = send(src, block, ring["y-"])

        def begin_z(self, first=None):
            block = self.at(zh, y)
            src = block if first is None else first
            self.zr = send(src, block, ring["z+"])
            self.zl = send(src, block, ring["z-"])

        def take_z_right(self):
            self.zr.wait_recv()
            half = self.at(self.origin[1], y, 0, HALF)
            self.zt = send(half, half, ring["z+"])

        def take_z_left(self):
            self.zl.wait_recv()
            half = self.at(self.origin[2], y, HALF, HALF)
            self.zb = send(half, half, ring["z-"])

        def take_z_far(self):
            self.zt.wait_recv()
            self.zb.wait_recv()

        def take_y(self, b):
            z = self.origin[b]
            self.right[b].wait_recv()
            half = self.at(z, wrap(y - 1), 0, HALF)
            self.tops[b] = send(half, half, ring["y+"])
            self.left[b].wait_recv()
            half = self.at(z, wrap(y + 1), HALF, HALF)
            self.bottoms[b] = send(half, half, ring["y-"])

        def take_y_far(self, b):
            self.tops[b].wait_recv()
            self.bottoms[b].wait_recv()

    class RingX:
        def __init__(self, at):
            self.at = at
            self.shared = []

        def begin(self):
            block = self.at(x, c)
            self.right = send(block, block, ring["x+"])
            self.left = send(block, block, ring["x-"])
            self.share(x)

        def share(self, origin):
            block = self.at(origin, c)
            self.shared.append(send(block, block, ring["core"]))

        def take(self):
            self.right.wait_recv()
            half = self.at(wrap(x - 1), c, 0, HALF)
            self.top = send(half, half, ring["x+"])
            self.left.wait_recv()
            half = self.at(wrap(x + 1), c, HALF, HALF)
            self.bottom = send(half, half, ring["x-"])
            self.share(wrap(x - 1))
            self.share(wrap(x + 1))

        def take_far(self):
            self.top.wait_recv()
            self.bottom.wait_recv()
            self.share(wrap(x + 2))

        def finish(self):
            for copy in self.shared:
                copy.wait_recv()

    local[2].wait()
    local[3].wait()
    own_hid = pl.ds(pl.multiple_of(dp * ROWS, 16), ROWS)
    hid[own_hid, :] = (sv[...].astype(jnp.float32) * uv[...].astype(jnp.float32)).astype(jnp.bfloat16)
    local[0].wait()
    local[1].wait()
    own_block = pltpu.make_async_copy(dyv, at_rows(zh, y), lsem.at[6])
    own_block.start()
    others = jnp.where(alone_x, 0, 1) + jnp.where(alone_d, 0, 1)
    pl.semaphore_wait(barrier, len(ring) + others)

    g_rows, g_x, g_d = Gather(at_rows), Gather(at_xt), Gather(at_dyt)
    g_rows.begin_z(dyv)
    g_rows.along_y(0, dyv)

    hid_own = RingX(lambda x, c, start=0, size=ROWS: rows_at(hid, x * 4 + zl * 2 + c, start, size))
    hid_pair = RingX(lambda x, c, start=0, size=ROWS: rows_at(hid, x * 4 + (1 - zl) * 2 + c, start, size))
    hid_own.begin()

    def transposed(src, dst, peer, alone, i):
        away = pltpu.make_async_remote_copy(
            src_ref=src, dst_ref=dst, send_sem=tsem.at[2 * i], recv_sem=tsem.at[2 * i + 1],
            device_id=peer, device_id_type=MESH,
        )
        here = pltpu.make_async_copy(src, dst, tsem.at[2 * i])

        @pl.when(jnp.logical_not(alone))
        def _():
            away.start()

        @pl.when(alone)
        def _():
            here.start()

        def wait():
            @pl.when(jnp.logical_not(alone))
            def _():
                away.wait()

            @pl.when(alone)
            def _():
                here.wait()

        return wait

    got_x = transposed(xv, at_xt(x, y1 * 2 + c), swap_x, alone_x, 0)
    got_d = transposed(dyv, rows_at(dyt, dp), swap_d, alone_d, 1)
    own = hid_own.at(x, c)
    pair = send(own, own, ring["pair"])

    local[4].wait()
    token = lax.broadcasted_iota(jnp.int32, (HALF, HALF), 0)
    place = lax.broadcasted_iota(jnp.int32, (HALF, HALF), 1)
    order = (place == lax.rem(token, 10) * 8 + token // 10).astype(jnp.float32).astype(jnp.bfloat16)
    for m in range(2):
        words = cv[m * 8 : m * 8 + 8, :]
        codes = jnp.concatenate(
            [jnp.bitwise_and(jnp.right_shift(words, 3 * k), 7).astype(jnp.float32) for k in range(10)], axis=0
        ).astype(jnp.bfloat16)
        codes = jnp.dot(order, codes, preferred_element_type=jnp.float32)
        level = jnp.full(codes.shape, SLOPE_LEVELS[0], jnp.float32)
        for symbol in range(1, 8):
            level = jnp.where(codes == jnp.float32(symbol), jnp.float32(SLOPE_LEVELS[symbol]), level)
        slopes[m * HALF : m * HALF + HALF, :] = level
    own_block.wait()
    local[5].wait()

    def multiply(z, y, first=False):
        block = at_rows(z, y)[...]
        weights = wv[:, pl.ds(pl.multiple_of((z * 4 + y) * BLOCK, BLOCK), BLOCK)]
        product = lax.dot_general(block, weights, (((1,), (1,)), ((), ())), preferred_element_type=jnp.float32)
        h[...] = product if first else h[...] + product

    multiply(zh, y, True)
    g_rows.take_z_right()
    g_rows.along_y(1)
    g_rows.take_z_left()
    g_rows.along_y(2)
    g_rows.take_y(0)
    g_rows.take_z_far()
    g_rows.along_y(3)
    got_x()
    g_x.begin_z()
    got_d()
    multiply(g_rows.origin[1], y)
    multiply(g_rows.origin[2], y)
    g_rows.take_y(1)
    multiply(g_rows.origin[3], y)
    multiply(zh, wrap(y - 1))
    multiply(zh, wrap(y + 1))
    hid_own.take()
    g_rows.take_y(2)
    multiply(g_rows.origin[1], wrap(y - 1))
    multiply(g_rows.origin[1], wrap(y + 1))
    pair.wait_recv()
    hid_pair.begin()
    g_x.take_z_right()
    g_x.take_z_left()
    g_x.take_z_far()
    g_d.begin_z()
    g_rows.take_y(3)
    for b in range(4):
        g_x.along_y(b)
    hid_own.take_far()
    g_rows.take_y_far(0)
    multiply(g_rows.origin[2], wrap(y - 1))
    multiply(g_rows.origin[2], wrap(y + 1))
    multiply(g_rows.origin[0], wrap(y + 2))
    g_rows.take_y_far(1)
    multiply(g_rows.origin[1], wrap(y + 2))
    multiply(g_rows.origin[3], wrap(y - 1))
    multiply(g_rows.origin[3], wrap(y + 1))
    g_rows.take_y_far(2)
    multiply(g_rows.origin[2], wrap(y + 2))
    g_rows.take_y_far(3)
    multiply(g_rows.origin[3], wrap(y + 2))

    def ring_of(k):
        return RingX(lambda x, c, start=0, size=ROWS: rows_at(gu.at[k], x * 2 + c, start, size))

    rings = [ring_of(k) for k in range(CHUNKS)]
    own_gu = pl.ds(pl.multiple_of((x * 2 + c) * ROWS, 16), ROWS)

    def activations(k):
        columns = slice(k * PART, (k + 1) * PART)
        grad = h[:, columns]
        gate = grad * uv[:, columns].astype(jnp.float32) * slopes[:, columns]
        gu[k, own_gu, 0:PART] = gate.astype(jnp.bfloat16)
        gu[k, own_gu, PART:WIDE] = (grad * sv[:, columns].astype(jnp.float32)).astype(jnp.bfloat16)

    for k in range(CHUNKS):
        activations(k)
        if k < 2:
            rings[k].begin()
    hid_pair.take()
    g_x.take_y(0)
    g_d.take_z_right()
    g_d.take_z_left()
    g_x.take_y(1)
    g_d.take_z_far()
    rings[0].take()
    g_x.take_y(2)
    rings[2].begin()
    g_x.take_y(3)
    hid_pair.take_far()
    for b in range(4):
        g_d.along_y(b)
    rings[1].take()
    rings[0].take_far()
    rings[3].begin()
    for b in range(4):
        g_x.take_y_far(b)
    for i in range(2):
        for r in range(5):
            xtt[i, :, r * 256 : (r + 1) * 256] = xt[i * 1280 + r * 256 : i * 1280 + (r + 1) * 256, :].T

    partials = []

    def products(k):
        rings[k].finish()
        values = gu[k]
        psend[k] = jnp.dot(xtt[1 - zl], values, preferred_element_type=jnp.float32).astype(jnp.bfloat16)
        partials.append(send(psend.at[k], precv.at[k], ring["pair"]))
        pown[k] = jnp.dot(xtt[zl], values, preferred_element_type=jnp.float32)

    def total(k):
        partials[k].wait_recv()
        whole = pown[k] + precv[k].astype(jnp.float32)
        columns = slice(k * PART, (k + 1) * PART)
        gate_ref[:, columns] = whole[:, 0:PART].astype(jnp.bfloat16)
        up_ref[:, columns] = whole[:, PART:WIDE].astype(jnp.bfloat16)

    products(0)
    rings[2].take()
    rings[1].take_far()
    g_d.take_y(0)
    products(1)
    rings[3].take()
    rings[2].take_far()
    g_d.take_y(1)
    g_d.take_y(2)
    products(2)
    g_d.take_y(3)
    rings[3].take_far()
    products(3)
    for b in range(4):
        g_d.take_y_far(b)
    hid_own.finish()
    hid_pair.finish()
    for r in range(10):
        dytt[:, r * 256 : (r + 1) * 256] = dyt[r * 256 : (r + 1) * 256, :].T
    for j in range(2):
        product = jnp.dot(dytt[...], hid[:, j * 512 : (j + 1) * 512], preferred_element_type=jnp.float32)
        down_ref[j * 512 : (j + 1) * 512, :] = product.T.astype(jnp.bfloat16)
    for k in range(CHUNKS):
        total(k)
    for copy in sent:
        copy.wait_send()


def shards(out_grad, layer_input, w_down, silu_gate, up_proj, slope_codes):
    bf16, f32 = jnp.bfloat16, jnp.float32
    vmem = pltpu.VMEM
    anywhere = pl.BlockSpec(memory_space=pl.ANY)
    down, gate, up = pl.pallas_call(
        kernel,
        out_shape=(
            jax.ShapeDtypeStruct((HIDDEN, BLOCK), bf16),
            jax.ShapeDtypeStruct((BLOCK, HIDDEN), bf16),
            jax.ShapeDtypeStruct((BLOCK, HIDDEN), bf16),
        ),
        in_specs=[anywhere] * 6,
        out_specs=[pl.BlockSpec(memory_space=pltpu.VMEM)] * 3,
        scratch_shapes=[
            vmem((ROWS, BLOCK), bf16),
            vmem((ROWS, BLOCK), bf16),
            vmem((HIDDEN, WIDTH), bf16),
            vmem((ROWS, HIDDEN), bf16),
            vmem((ROWS, HIDDEN), bf16),
            vmem((16, HIDDEN), jnp.int32),
            vmem((16 * ROWS, BLOCK), bf16),
            vmem((16 * ROWS, BLOCK), bf16),
            vmem((16 * ROWS, BLOCK), bf16),
            vmem((16 * ROWS, HIDDEN), bf16),
            vmem((CHUNKS, 8 * ROWS, WIDE), bf16),
            vmem((ROWS, HIDDEN), f32),
            vmem((ROWS, HIDDEN), f32),
            vmem((2, BLOCK, 8 * ROWS), bf16),
            vmem((BLOCK, 16 * ROWS), bf16),
            vmem((CHUNKS, BLOCK, WIDE), bf16),
            vmem((CHUNKS, BLOCK, WIDE), bf16),
            vmem((CHUNKS, BLOCK, WIDE), f32),
            pltpu.SemaphoreType.DMA((8,)),
            pltpu.SemaphoreType.DMA((N_COPIES,)),
            pltpu.SemaphoreType.DMA((N_COPIES,)),
            pltpu.SemaphoreType.DMA((4,)),
        ],
        compiler_params=pltpu.CompilerParams(
            collective_id=0, has_side_effects=True, vmem_limit_bytes=62 * 1024 * 1024
        ),
    )(
        out_grad.reshape(ROWS, BLOCK),
        layer_input.reshape(ROWS, BLOCK),
        w_down,
        silu_gate.reshape(ROWS, HIDDEN),
        up_proj.reshape(ROWS, HIDDEN),
        slope_codes.reshape(16, HIDDEN),
    )
    return down, gate, up


def solution(mesh):
    return jax.shard_map(
        shards,
        mesh=mesh,
        in_specs=(
            P(None, "dp", "tensor"),
            P(None, "dp", "tensor"),
            P("tensor", None),
            P(None, "dp", "tensor"),
            P(None, "dp", "tensor"),
            P(None, "dp", "tensor"),
        ),
        out_specs=(P("tensor", "dp"), P("dp", "tensor"), P("dp", "tensor")),
        check_vma=False,
    )
```

```python
import jax
import jax.numpy as jnp
from jax import lax
from jax.experimental import pallas as pl
from jax.experimental.pallas import tpu as pltpu
from jax.sharding import PartitionSpec as P

SLOPE_LEVELS = (-0.09, 0.06, 0.22, 0.41, 0.6, 0.79, 0.96, 1.08)
MESH = pl.DeviceIdType.MESH
ROWS = 160
HALF = 80
BLOCK = 256
HIDDEN = 1024
WIDTH = 4096
CHUNKS = 4
DOWN = 2
PIECES = DOWN + CHUNKS
PART = HIDDEN // CHUNKS
WIDE = 2 * PART
N_COPIES = 128


def wrap(value):
    return lax.rem(value + 4, 4)


def kernel(
    dy_hbm, x_hbm, w_hbm, s_hbm, u_hbm, code_hbm,
    down_hbm, gate_hbm, up_hbm,
    wv, sv, uv, cv, rows, xz, xt, dyt, relays, gu, h, slopes, xtt, dytt, psend, precv, pown,
    down_ref, gate_ref, up_ref, lsem, osem, ssem, rsem,
):
    dp = lax.axis_index("dp")
    tensor = lax.axis_index("tensor")
    x, zl, c = dp // 4, lax.rem(dp // 2, 2), lax.rem(dp, 2)
    zh, y = tensor // 4, lax.rem(tensor, 4)

    def device(x=x, zl=zl, c=c, zh=zh, y=y):
        return {"dp": x * 4 + zl * 2 + c, "tensor": zh * 4 + y}

    ring = {
        "x+": device(x=wrap(x + 1)), "x-": device(x=wrap(x - 1)),
        "y+": device(y=wrap(y + 1)), "y-": device(y=wrap(y - 1)),
        "z+": device(zh=wrap(zh + 1)), "z-": device(zh=wrap(zh - 1)),
        "core": device(c=1 - c), "pair": device(zl=1 - zl),
    }

    barrier = pltpu.get_barrier_semaphore()
    for peer in ring.values():
        pl.semaphore_signal(barrier, inc=1, device_id=peer, device_id_type=MESH)

    def rows_at(buffer, row, start=0, size=ROWS):
        return buffer.at[pl.ds(pl.multiple_of(row * ROWS + start, 16), size)]

    def at_rows(zh, y, start=0, size=ROWS):
        return rows_at(rows, zh * 4 + y, start, size)

    def at_xz(zh, y, start=0, size=ROWS):
        return rows_at(xz, zh, start, size)

    local = [
        pltpu.make_async_copy(src, dst, lsem.at[i])
        for i, (src, dst) in enumerate((
            (dy_hbm, at_rows(zh, y)), (x_hbm, at_xz(zh, y)), (s_hbm, sv), (u_hbm, uv), (code_hbm, cv), (w_hbm, wv)
        ))
    ]
    for copy in local:
        copy.start()

    sent = []

    def send(src, dst, peer):
        i = len(sent)
        copy = pltpu.make_async_remote_copy(
            src_ref=src, dst_ref=dst, send_sem=ssem.at[i], recv_sem=rsem.at[i],
            device_id=ring[peer], device_id_type=MESH,
        )
        copy.start()
        sent.append(copy)
        return copy

    class Ring:
        def __init__(self, at, me, axis):
            self.at, self.me, self.up, self.down = at, me, axis + "+", axis + "-"

        def begin(self, src=None):
            block = self.at(self.me)
            src = block if src is None else src
            self.right = send(src, block, self.up)
            self.left = send(src, block, self.down)

        def take(self):
            self.right.wait_recv()
            half = self.at(wrap(self.me - 1), 0, HALF)
            self.top = send(half, half, self.up)
            self.left.wait_recv()
            half = self.at(wrap(self.me + 1), HALF, HALF)
            self.bottom = send(half, half, self.down)

        def take_far(self):
            self.top.wait_recv()
            self.bottom.wait_recv()

    class Turn:
        def __init__(self, source, buffer, i):
            self.source, self.buffer, self.relay, self.i = source, buffer, relays.at[i], i
            self.origin = (x, wrap(x - 1), wrap(x + 1), wrap(x + 2))
            self.over_y = [
                Ring(lambda yo, start=0, size=ROWS, o=o: self.at(yo, o, start, size), y, "y") for o in self.origin
            ]

        def at(self, yo, xo, start=0, size=ROWS):
            return rows_at(self.buffer, yo * 8 + c * 4 + xo, start, size)

        def begin(self):
            self.kept = pltpu.make_async_copy(self.source(x), self.at(y, x), lsem.at[6 + self.i])
            self.kept.start()
            self.far_top = send(self.source(wrap(x + 2), 0, HALF), self.relay.at[0], "x+")
            self.far_bottom = send(self.source(wrap(x + 2), HALF, HALF), self.relay.at[1], "x-")
            self.right = send(self.source(wrap(x + 1)), self.at(y, x), "x+")
            self.left = send(self.source(wrap(x - 1)), self.at(y, x), "x-")

        def pass_on(self):
            self.far_top.wait_recv()
            self.top = send(self.relay.at[0], self.at(y, wrap(x - 1), 0, HALF), "x+")
            self.far_bottom.wait_recv()
            self.bottom = send(self.relay.at[1], self.at(y, wrap(x + 1), HALF, HALF), "x-")

        def along_y(self, b):
            if b == 0:
                self.kept.wait()
            elif b == 1:
                self.right.wait_recv()
            elif b == 2:
                self.left.wait_recv()
            else:
                self.top.wait_recv()
                self.bottom.wait_recv()
            self.over_y[b].begin()

        def share(self):
            self.shared = []
            for yo in (1 - c, 3 - c):
                block = self.buffer.at[pl.ds(pl.multiple_of((yo * 8 + c * 4) * ROWS, 16), 4 * ROWS)]
                self.shared.append(send(block, block, "core"))

        def finish(self):
            for copy in self.shared:
                copy.wait_recv()

        def turn(self, out):
            for i in range(2):
                for r in range(5):
                    start = pl.multiple_of((2 * i + c) * (8 * ROWS) + r * 256, 256)
                    out[i, :, r * 256 : (r + 1) * 256] = self.buffer[pl.ds(start, 256), :].T

    class Piece:
        def __init__(self, k):
            self.over_x = Ring(self.at(k), x, "x")
            self.shared = []

        def at(self, k):
            return lambda xo, start=0, size=ROWS: rows_at(gu.at[k], c * 4 + xo, start, size)

        def share(self, origin):
            block = self.over_x.at(origin)
            self.shared.append(send(block, block, "core"))

        def begin(self):
            self.over_x.begin()
            self.share(x)

        def take(self):
            self.over_x.take()
            self.share(wrap(x - 1))
            self.share(wrap(x + 1))

        def take_far(self):
            self.over_x.take_far()
            self.share(wrap(x + 2))

        def finish(self):
            for copy in self.shared:
                copy.wait_recv()

    own_rows = pl.ds(pl.multiple_of((c * 4 + x) * ROWS, 16), ROWS)
    local[2].wait()
    local[3].wait()
    for k in range(DOWN):
        columns = slice(k * WIDE, (k + 1) * WIDE)
        gu[k, own_rows, :] = (sv[:, columns].astype(jnp.float32) * uv[:, columns].astype(jnp.float32)).astype(jnp.bfloat16)
    local[0].wait()
    local[1].wait()
    pl.semaphore_wait(barrier, len(ring))

    origins = (zh, wrap(zh - 1), wrap(zh + 1), wrap(zh + 2))
    rows_z = Ring(lambda zo, start=0, size=ROWS: at_rows(zo, y, start, size), zh, "z")
    rows_y = [Ring(lambda yo, start=0, size=ROWS, o=o: at_rows(o, yo, start, size), y, "y") for o in origins]
    x_z = Ring(lambda zo, start=0, size=ROWS: at_xz(zo, y, start, size), zh, "z")
    turn_d = Turn(lambda zo, start=0, size=ROWS: at_rows(zo, y, start, size), dyt, 0)
    turn_x = Turn(lambda zo, start=0, size=ROWS: at_xz(zo, y, start, size), xt, 1)
    pieces = [Piece(k) for k in range(PIECES)]

    rows_z.begin()
    rows_y[0].begin()
    pieces[0].begin()
    pieces[1].begin()

    local[4].wait()
    token = lax.broadcasted_iota(jnp.int32, (HALF, HALF), 0)
    place = lax.broadcasted_iota(jnp.int32, (HALF, HALF), 1)
    order = (place == lax.rem(token, 10) * 8 + token // 10).astype(jnp.float32).astype(jnp.bfloat16)
    for m in range(2):
        words = cv[m * 8 : m * 8 + 8, :]
        codes = jnp.concatenate(
            [jnp.bitwise_and(jnp.right_shift(words, 3 * k), 7).astype(jnp.float32) for k in range(10)], axis=0
        ).astype(jnp.bfloat16)
        codes = jnp.dot(order, codes, preferred_element_type=jnp.float32)
        level = jnp.full(codes.shape, SLOPE_LEVELS[0], jnp.float32)
        for symbol in range(1, 8):
            level = jnp.where(codes == jnp.float32(symbol), jnp.float32(SLOPE_LEVELS[symbol]), level)
        slopes[m * HALF : m * HALF + HALF, :] = level
    local[5].wait()

    def multiply(b, yo, first=False):
        z = origins[b]
        weights = wv[:, pl.ds(pl.multiple_of((z * 4 + yo) * BLOCK, BLOCK), BLOCK)]
        product = lax.dot_general(
            at_rows(z, yo)[...], weights, (((1,), (1,)), ((), ())), preferred_element_type=jnp.float32
        )
        h[...] = product if first else h[...] + product

    def activations(k):
        columns = slice(k * PART, (k + 1) * PART)
        grad = h[:, columns]
        gate = grad * uv[:, columns].astype(jnp.float32) * slopes[:, columns]
        gu[DOWN + k, own_rows, 0:PART] = gate.astype(jnp.bfloat16)
        gu[DOWN + k, own_rows, PART:WIDE] = (grad * sv[:, columns].astype(jnp.float32)).astype(jnp.bfloat16)

    partials = {}
    outward = []

    def products(k):
        pieces[k].finish()
        lhs = dytt if k < DOWN else xtt
        values = gu[k]
        psend[k] = jnp.dot(lhs[1 - zl], values, preferred_element_type=jnp.float32).astype(jnp.bfloat16)
        partials[k] = send(psend.at[k], precv.at[k], "pair")
        pown[k] = jnp.dot(lhs[zl], values, preferred_element_type=jnp.float32)

    def put(src, dst):
        copy = pltpu.make_async_copy(src, dst, osem.at[len(outward)])
        copy.start()
        outward.append(copy)

    def total(k):
        partials[k].wait_recv()
        whole = pown[k] + precv[k].astype(jnp.float32)
        if k < DOWN:
            part = slice(k * WIDE, (k + 1) * WIDE)
            down_ref[part, :] = whole.T.astype(jnp.bfloat16)
            put(down_ref.at[part], down_hbm.at[part])
        else:
            part = slice((k - DOWN) * PART, (k - DOWN + 1) * PART)
            gate_ref[:, part] = whole[:, 0:PART].astype(jnp.bfloat16)
            put(gate_ref.at[:, part], gate_hbm.at[:, part])
            up_ref[:, part] = whole[:, PART:WIDE].astype(jnp.bfloat16)
            put(up_ref.at[:, part], up_hbm.at[:, part])

    multiply(0, y, True)
    rows_z.take()
    rows_y[1].begin()
    rows_y[2].begin()
    x_z.begin()
    rows_y[0].take()
    multiply(1, y)
    multiply(2, y)
    rows_z.take_far()
    rows_y[3].begin()
    turn_d.begin()
    pieces[0].take()
    multiply(3, y)
    multiply(0, wrap(y - 1))
    multiply(0, wrap(y + 1))
    rows_y[1].take()
    x_z.take()
    multiply(1, wrap(y - 1))
    multiply(1, wrap(y + 1))
    turn_d.pass_on()
    pieces[1].take()
    rows_y[2].take()
    multiply(2, wrap(y - 1))
    multiply(2, wrap(y + 1))
    x_z.take_far()
    turn_x.begin()
    rows_y[3].take()
    turn_d.along_y(0)
    turn_d.along_y(1)
    turn_d.along_y(2)
    turn_d.along_y(3)
    pieces[0].take_far()
    multiply(3, wrap(y - 1))
    multiply(3, wrap(y + 1))
    for b in range(4):
        rows_y[b].take_far()
        multiply(b, wrap(y + 2))
    for k in range(CHUNKS):
        activations(k)
        if k < 2:
            pieces[DOWN + k].begin()
    turn_x.pass_on()
    pieces[1].take_far()
    turn_d.over_y[0].take()
    turn_d.over_y[1].take()
    turn_x.along_y(0)
    turn_x.along_y(1)
    turn_d.over_y[2].take()
    turn_x.along_y(2)
    turn_d.over_y[3].take()
    turn_x.along_y(3)
    pieces[2].take()
    pieces[4].begin()
    for b in range(4):
        turn_d.over_y[b].take_far()
    turn_d.share()
    pieces[3].take()
    turn_x.over_y[0].take()
    turn_d.finish()
    turn_d.turn(dytt)
    products(0)
    pieces[2].take_far()
    pieces[5].begin()
    turn_x.over_y[1].take()
    products(1)
    turn_x.over_y[2].take()
    turn_x.over_y[3].take()
    pieces[4].take()
    pieces[3].take_far()
    for b in range(4):
        turn_x.over_y[b].take_far()
    turn_x.share()
    pieces[5].take()
    turn_x.finish()
    turn_x.turn(xtt)
    products(2)
    pieces[4].take_far()
    products(3)
    pieces[5].take_far()
    products(4)
    products(5)
    for k in range(PIECES):
        total(k)
    for copy in outward:
        copy.wait()
    for copy in sent:
        copy.wait_send()


def hand_over(*refs):
    for src, dst in zip(refs[:3], refs[3:]):
        dst[...] = src[...]


def shards(out_grad, layer_input, w_down, silu_gate, up_proj, slope_codes):
    bf16, f32 = jnp.bfloat16, jnp.float32
    vmem = pltpu.VMEM
    anywhere = pl.BlockSpec(memory_space=pl.ANY)
    results = pl.pallas_call(
        kernel,
        out_shape=(
            jax.ShapeDtypeStruct((HIDDEN, BLOCK), bf16),
            jax.ShapeDtypeStruct((BLOCK, HIDDEN), bf16),
            jax.ShapeDtypeStruct((BLOCK, HIDDEN), bf16),
        ),
        in_specs=[pl.BlockSpec(memory_space=pltpu.HBM)] * 6,
        out_specs=[anywhere] * 3,
        scratch_shapes=[
            vmem((HIDDEN, WIDTH), bf16),
            vmem((ROWS, HIDDEN), bf16),
            vmem((ROWS, HIDDEN), bf16),
            vmem((16, HIDDEN), jnp.int32),
            vmem((16 * ROWS, BLOCK), bf16),
            vmem((4 * ROWS, BLOCK), bf16),
            vmem((32 * ROWS, BLOCK), bf16),
            vmem((32 * ROWS, BLOCK), bf16),
            vmem((2, 2, HALF, BLOCK), bf16),
            vmem((PIECES, 8 * ROWS, WIDE), bf16),
            vmem((ROWS, HIDDEN), f32),
            vmem((ROWS, HIDDEN), f32),
            vmem((2, BLOCK, 8 * ROWS), bf16),
            vmem((2, BLOCK, 8 * ROWS), bf16),
            vmem((PIECES, BLOCK, WIDE), bf16),
            vmem((PIECES, BLOCK, WIDE), bf16),
            vmem((PIECES, BLOCK, WIDE), f32),
            vmem((HIDDEN, BLOCK), bf16),
            vmem((BLOCK, HIDDEN), bf16),
            vmem((BLOCK, HIDDEN), bf16),
            pltpu.SemaphoreType.DMA((8,)),
            pltpu.SemaphoreType.DMA((2 * CHUNKS + DOWN,)),
            pltpu.SemaphoreType.DMA((N_COPIES,)),
            pltpu.SemaphoreType.DMA((N_COPIES,)),
        ],
        compiler_params=pltpu.CompilerParams(
            collective_id=0, has_side_effects=True, vmem_limit_bytes=44 * 1024 * 1024
        ),
    )(
        out_grad.reshape(ROWS, BLOCK),
        layer_input.reshape(ROWS, BLOCK),
        w_down,
        silu_gate.reshape(ROWS, HIDDEN),
        up_proj.reshape(ROWS, HIDDEN),
        slope_codes.reshape(16, HIDDEN),
    )
    return pl.pallas_call(
        hand_over,
        out_shape=tuple(jax.ShapeDtypeStruct(a.shape, a.dtype) for a in results),
        in_specs=[pl.BlockSpec(memory_space=pltpu.VMEM)] * 3,
        out_specs=[pl.BlockSpec(memory_space=pltpu.VMEM)] * 3,
        compiler_params=pltpu.CompilerParams(vmem_limit_bytes=8 * 1024 * 1024),
    )(*results)


def solution(mesh):
    return jax.shard_map(
        shards,
        mesh=mesh,
        in_specs=(
            P(None, "dp", "tensor"),
            P(None, "dp", "tensor"),
            P("tensor", None),
            P(None, "dp", "tensor"),
            P(None, "dp", "tensor"),
            P(None, "dp", "tensor"),
        ),
        out_specs=(P("tensor", "dp"), P("dp", "tensor"), P("dp", "tensor")),
        check_vma=False,
    )
```

```python
import jax
import jax.numpy as jnp
from jax import lax
from jax.experimental import pallas as pl
from jax.experimental.pallas import tpu as pltpu
from jax.sharding import PartitionSpec as P

SLOPE_LEVELS = (-0.09, 0.06, 0.22, 0.41, 0.6, 0.79, 0.96, 1.08)
MESH = pl.DeviceIdType.MESH
ROWS = 160
HALF = 80
BLOCK = 256
HIDDEN = 1024
WIDTH = 4096
CHUNKS = 4
DOWN = 2
PIECES = DOWN + CHUNKS
PART = HIDDEN // CHUNKS
WIDE = 2 * PART
N_COPIES = 160


def wrap(value):
    return lax.rem(value + 4, 4)


def kernel(
    dy_hbm, x_hbm, w_hbm, s_hbm, u_hbm, code_hbm,
    down_hbm, gate_hbm, up_hbm,
    wv, sv, uv, cv, rows, xz, xt, dyt, relays, gu, h, slopes, xtt, dytt, psend, precv, pown,
    down_ref, gate_ref, up_ref, lsem, osem, ssem, rsem,
):
    dp = lax.axis_index("dp")
    tensor = lax.axis_index("tensor")
    x, zl, c = dp // 4, lax.rem(dp // 2, 2), lax.rem(dp, 2)
    zh, y = tensor // 4, lax.rem(tensor, 4)

    def device(x=x, zl=zl, c=c, zh=zh, y=y):
        return {"dp": x * 4 + zl * 2 + c, "tensor": zh * 4 + y}

    ring = {
        "x+": device(x=wrap(x + 1)), "x-": device(x=wrap(x - 1)),
        "y+": device(y=wrap(y + 1)), "y-": device(y=wrap(y - 1)),
        "z+": device(zh=wrap(zh + 1)), "z-": device(zh=wrap(zh - 1)),
        "core": device(c=1 - c), "pair": device(zl=1 - zl),
    }

    barrier = pltpu.get_barrier_semaphore()
    for peer in ring.values():
        pl.semaphore_signal(barrier, inc=1, device_id=peer, device_id_type=MESH)

    def rows_at(buffer, row, start=0, size=ROWS):
        return buffer.at[pl.ds(pl.multiple_of(row * ROWS + start, 16), size)]

    def at_rows(zh, y, start=0, size=ROWS):
        return rows_at(rows, zh * 4 + y, start, size)

    def at_xz(zh, y, start=0, size=ROWS):
        return rows_at(xz, zh, start, size)

    local = [
        pltpu.make_async_copy(src, dst, lsem.at[i])
        for i, (src, dst) in enumerate((
            (dy_hbm, at_rows(zh, y)), (x_hbm, at_xz(zh, y)), (s_hbm, sv), (u_hbm, uv), (code_hbm, cv), (w_hbm, wv)
        ))
    ]
    for copy in local:
        copy.start()

    sent = []

    def send(src, dst, peer):
        i = len(sent)
        copy = pltpu.make_async_remote_copy(
            src_ref=src, dst_ref=dst, send_sem=ssem.at[i], recv_sem=rsem.at[i],
            device_id=ring[peer], device_id_type=MESH,
        )
        copy.start()
        sent.append(copy)
        return copy

    class Ring:
        def __init__(self, at, me, axis, split=False):
            self.at, self.me, self.up, self.down, self.split = at, me, axis + "+", axis + "-", split

        def begin(self):
            if self.split:
                top, bottom = self.at(self.me, 0, HALF), self.at(self.me, HALF, HALF)
                self.right = send(top, top, self.up)
                self.left = send(bottom, bottom, self.down)
                self.rest = (send(bottom, bottom, self.up), send(top, top, self.down))
            else:
                block = self.at(self.me)
                self.right = send(block, block, self.up)
                self.left = send(block, block, self.down)
                self.rest = ()

        def take(self):
            self.right.wait_recv()
            half = self.at(wrap(self.me - 1), 0, HALF)
            self.top = send(half, half, self.up)
            self.left.wait_recv()
            half = self.at(wrap(self.me + 1), HALF, HALF)
            self.bottom = send(half, half, self.down)
            for copy in self.rest:
                copy.wait_recv()

        def take_far(self):
            self.top.wait_recv()
            self.bottom.wait_recv()

    class Turn:
        def __init__(self, source, buffer, i):
            self.source, self.buffer, self.relay, self.i = source, buffer, relays.at[i], i
            self.origin = (x, wrap(x - 1), wrap(x + 1), wrap(x + 2))
            self.shared = []
            self.over_y = [
                Ring(lambda yo, start=0, size=ROWS, o=o: self.at(yo, o, start, size), y, "y") for o in self.origin
            ]

        def at(self, yo, xo, start=0, size=ROWS):
            return rows_at(self.buffer, yo * 8 + c * 4 + xo, start, size)

        def begin(self):
            self.kept = pltpu.make_async_copy(self.source(x), self.at(y, x), lsem.at[6 + self.i])
            self.kept.start()
            self.far_top = send(self.source(wrap(x + 2), 0, HALF), self.relay.at[0], "x+")
            self.far_bottom = send(self.source(wrap(x + 2), HALF, HALF), self.relay.at[1], "x-")
            self.right = send(self.source(wrap(x + 1)), self.at(y, x), "x+")
            self.left = send(self.source(wrap(x - 1)), self.at(y, x), "x-")

        def pass_on(self):
            self.far_top.wait_recv()
            self.top = send(self.relay.at[0], self.at(y, wrap(x - 1), 0, HALF), "x+")
            self.far_bottom.wait_recv()
            self.bottom = send(self.relay.at[1], self.at(y, wrap(x + 1), HALF, HALF), "x-")

        def along_y(self, b):
            if b == 0:
                self.kept.wait()
            elif b == 1:
                self.right.wait_recv()
            elif b == 2:
                self.left.wait_recv()
            else:
                self.top.wait_recv()
                self.bottom.wait_recv()
            self.over_y[b].begin()

        def arrive(self, b):
            self.over_y[b].take_far()
            for yo in (1 - c, 3 - c):
                block = self.at(yo, self.origin[b])
                self.shared.append(send(block, block, "core"))

        def finish(self):
            for copy in self.shared:
                copy.wait_recv()

        def turn(self, out):
            for i in range(2):
                for r in range(5):
                    start = pl.multiple_of((2 * i + c) * (8 * ROWS) + r * 256, 256)
                    out[i, :, r * 256 : (r + 1) * 256] = self.buffer[pl.ds(start, 256), :].T

    class Piece:
        def __init__(self, k):
            self.over_x = Ring(self.at(k), x, "x")
            self.shared = []

        def at(self, k):
            return lambda xo, start=0, size=ROWS: rows_at(gu.at[k], c * 4 + xo, start, size)

        def share(self, origin):
            block = self.over_x.at(origin)
            self.shared.append(send(block, block, "core"))

        def begin(self):
            self.over_x.begin()
            self.share(x)

        def take(self):
            self.over_x.take()
            self.share(wrap(x - 1))
            self.share(wrap(x + 1))

        def take_far(self):
            self.over_x.take_far()
            self.share(wrap(x + 2))

        def finish(self):
            for copy in self.shared:
                copy.wait_recv()

    own_rows = pl.ds(pl.multiple_of((c * 4 + x) * ROWS, 16), ROWS)
    local[2].wait()
    local[3].wait()
    for k in range(DOWN):
        columns = slice(k * WIDE, (k + 1) * WIDE)
        gu[k, own_rows, :] = (sv[:, columns].astype(jnp.float32) * uv[:, columns].astype(jnp.float32)).astype(jnp.bfloat16)
    local[0].wait()
    local[1].wait()
    pl.semaphore_wait(barrier, len(ring))

    origins = (zh, wrap(zh - 1), wrap(zh + 1), wrap(zh + 2))
    rows_z = Ring(lambda zo, start=0, size=ROWS: at_rows(zo, y, start, size), zh, "z", True)
    rows_y = [Ring(lambda yo, start=0, size=ROWS, o=o: at_rows(o, yo, start, size), y, "y") for o in origins]
    x_z = Ring(lambda zo, start=0, size=ROWS: at_xz(zo, y, start, size), zh, "z", True)
    turn_d = Turn(lambda zo, start=0, size=ROWS: at_rows(zo, y, start, size), dyt, 0)
    turn_x = Turn(lambda zo, start=0, size=ROWS: at_xz(zo, y, start, size), xt, 1)
    pieces = [Piece(k) for k in range(PIECES)]

    rows_z.begin()
    rows_y[0].begin()
    pieces[0].begin()
    pieces[1].begin()

    local[4].wait()
    token = lax.broadcasted_iota(jnp.int32, (HALF, HALF), 0)
    place = lax.broadcasted_iota(jnp.int32, (HALF, HALF), 1)
    order = (place == lax.rem(token, 10) * 8 + token // 10).astype(jnp.float32).astype(jnp.bfloat16)
    for m in range(2):
        words = cv[m * 8 : m * 8 + 8, :]
        codes = jnp.concatenate(
            [jnp.bitwise_and(jnp.right_shift(words, 3 * k), 7).astype(jnp.float32) for k in range(10)], axis=0
        ).astype(jnp.bfloat16)
        codes = jnp.dot(order, codes, preferred_element_type=jnp.float32)
        level = jnp.full(codes.shape, SLOPE_LEVELS[0], jnp.float32)
        for symbol in range(1, 8):
            level = jnp.where(codes == jnp.float32(symbol), jnp.float32(SLOPE_LEVELS[symbol]), level)
        slopes[m * HALF : m * HALF + HALF, :] = level
    local[5].wait()

    def multiply(b, yo, first=False):
        z = origins[b]
        weights = wv[:, pl.ds(pl.multiple_of((z * 4 + yo) * BLOCK, BLOCK), BLOCK)]
        product = lax.dot_general(
            at_rows(z, yo)[...], weights, (((1,), (1,)), ((), ())), preferred_element_type=jnp.float32
        )
        h[...] = product if first else h[...] + product

    def activations(k):
        columns = slice(k * PART, (k + 1) * PART)
        grad = h[:, columns]
        gate = grad * uv[:, columns].astype(jnp.float32) * slopes[:, columns]
        gu[DOWN + k, own_rows, 0:PART] = gate.astype(jnp.bfloat16)
        gu[DOWN + k, own_rows, PART:WIDE] = (grad * sv[:, columns].astype(jnp.float32)).astype(jnp.bfloat16)

    partials = {}
    outward = []

    def products(k):
        pieces[k].finish()
        lhs = dytt if k < DOWN else xtt
        values = gu[k]
        psend[k] = jnp.dot(lhs[1 - zl], values, preferred_element_type=jnp.float32).astype(jnp.bfloat16)
        partials[k] = send(psend.at[k], precv.at[k], "pair")
        pown[k] = jnp.dot(lhs[zl], values, preferred_element_type=jnp.float32)

    def put(src, dst):
        copy = pltpu.make_async_copy(src, dst, osem.at[len(outward)])
        copy.start()
        outward.append(copy)

    def total(k):
        partials[k].wait_recv()
        whole = pown[k] + precv[k].astype(jnp.float32)
        if k < DOWN:
            part = slice(k * WIDE, (k + 1) * WIDE)
            down_ref[part, :] = whole.T.astype(jnp.bfloat16)
            put(down_ref.at[part], down_hbm.at[part])
        else:
            part = slice((k - DOWN) * PART, (k - DOWN + 1) * PART)
            gate_ref[:, part] = whole[:, 0:PART].astype(jnp.bfloat16)
            put(gate_ref.at[:, part], gate_hbm.at[:, part])
            up_ref[:, part] = whole[:, PART:WIDE].astype(jnp.bfloat16)
            put(up_ref.at[:, part], up_hbm.at[:, part])

    multiply(0, y, True)
    rows_z.take()
    rows_y[1].begin()
    rows_y[2].begin()
    x_z.begin()
    rows_y[0].take()
    multiply(1, y)
    multiply(2, y)
    rows_z.take_far()
    turn_d.begin()
    rows_y[3].begin()
    multiply(3, y)
    multiply(0, wrap(y - 1))
    multiply(0, wrap(y + 1))
    rows_y[1].take()
    turn_d.along_y(0)
    multiply(1, wrap(y - 1))
    multiply(1, wrap(y + 1))
    rows_y[2].take()
    turn_d.pass_on()
    turn_d.along_y(1)
    turn_d.along_y(2)
    x_z.take()
    rows_y[3].take()
    multiply(2, wrap(y - 1))
    multiply(2, wrap(y + 1))
    turn_d.over_y[0].take()
    turn_d.along_y(3)
    pieces[0].take()
    x_z.take_far()
    turn_x.begin()
    multiply(3, wrap(y - 1))
    multiply(3, wrap(y + 1))
    for b in range(3):
        rows_y[b].take_far()
        multiply(b, wrap(y + 2))
    turn_d.over_y[1].take()
    turn_d.over_y[2].take()
    pieces[1].take()
    turn_x.pass_on()
    turn_d.arrive(0)
    rows_y[3].take_far()
    multiply(3, wrap(y + 2))
    activations(0)
    pieces[2].begin()
    turn_d.over_y[3].take()
    activations(1)
    pieces[3].begin()
    turn_x.along_y(0)
    turn_x.along_y(1)
    pieces[0].take_far()
    turn_x.along_y(2)
    turn_d.arrive(1)
    turn_d.arrive(2)
    activations(2)
    activations(3)
    pieces[1].take_far()
    turn_d.arrive(3)
    turn_x.over_y[0].take()
    turn_d.finish()
    turn_d.turn(dytt)
    products(0)
    turn_x.along_y(3)
    pieces[2].take()
    products(1)
    pieces[4].begin()
    turn_x.over_y[1].take()
    turn_x.over_y[2].take()
    pieces[3].take()
    turn_x.over_y[3].take()
    turn_x.arrive(0)
    pieces[2].take_far()
    pieces[5].begin()
    turn_x.arrive(1)
    turn_x.arrive(2)
    pieces[4].take()
    turn_x.arrive(3)
    turn_x.finish()
    turn_x.turn(xtt)
    products(2)
    pieces[3].take_far()
    pieces[5].take()
    products(3)
    pieces[4].take_far()
    products(4)
    total(0)
    total(1)
    pieces[5].take_far()
    products(5)
    for k in range(DOWN, PIECES):
        total(k)
    for copy in outward:
        copy.wait()
    for copy in sent:
        copy.wait_send()


def hand_over(*refs):
    for src, dst in zip(refs[:3], refs[3:]):
        dst[...] = src[...]


def shards(out_grad, layer_input, w_down, silu_gate, up_proj, slope_codes):
    bf16, f32 = jnp.bfloat16, jnp.float32
    vmem = pltpu.VMEM
    anywhere = pl.BlockSpec(memory_space=pl.ANY)
    results = pl.pallas_call(
        kernel,
        out_shape=(
            jax.ShapeDtypeStruct((HIDDEN, BLOCK), bf16),
            jax.ShapeDtypeStruct((BLOCK, HIDDEN), bf16),
            jax.ShapeDtypeStruct((BLOCK, HIDDEN), bf16),
        ),
        in_specs=[pl.BlockSpec(memory_space=pltpu.HBM)] * 6,
        out_specs=[anywhere] * 3,
        scratch_shapes=[
            vmem((HIDDEN, WIDTH), bf16),
            vmem((ROWS, HIDDEN), bf16),
            vmem((ROWS, HIDDEN), bf16),
            vmem((16, HIDDEN), jnp.int32),
            vmem((16 * ROWS, BLOCK), bf16),
            vmem((4 * ROWS, BLOCK), bf16),
            vmem((32 * ROWS, BLOCK), bf16),
            vmem((32 * ROWS, BLOCK), bf16),
            vmem((2, 2, HALF, BLOCK), bf16),
            vmem((PIECES, 8 * ROWS, WIDE), bf16),
            vmem((ROWS, HIDDEN), f32),
            vmem((ROWS, HIDDEN), f32),
            vmem((2, BLOCK, 8 * ROWS), bf16),
            vmem((2, BLOCK, 8 * ROWS), bf16),
            vmem((PIECES, BLOCK, WIDE), bf16),
            vmem((PIECES, BLOCK, WIDE), bf16),
            vmem((PIECES, BLOCK, WIDE), f32),
            vmem((HIDDEN, BLOCK), bf16),
            vmem((BLOCK, HIDDEN), bf16),
            vmem((BLOCK, HIDDEN), bf16),
            pltpu.SemaphoreType.DMA((8,)),
            pltpu.SemaphoreType.DMA((2 * CHUNKS + DOWN,)),
            pltpu.SemaphoreType.DMA((N_COPIES,)),
            pltpu.SemaphoreType.DMA((N_COPIES,)),
        ],
        compiler_params=pltpu.CompilerParams(
            collective_id=0, has_side_effects=True, vmem_limit_bytes=44 * 1024 * 1024
        ),
    )(
        *(
            pltpu.with_memory_space_constraint(a, pltpu.HBM)
            for a in (
                out_grad.reshape(ROWS, BLOCK),
                layer_input.reshape(ROWS, BLOCK),
                w_down,
                silu_gate.reshape(ROWS, HIDDEN),
                up_proj.reshape(ROWS, HIDDEN),
                slope_codes.reshape(16, HIDDEN),
            )
        )
    )
    return pl.pallas_call(
        hand_over,
        out_shape=tuple(jax.ShapeDtypeStruct(a.shape, a.dtype) for a in results),
        in_specs=[pl.BlockSpec(memory_space=pltpu.VMEM)] * 3,
        out_specs=[pl.BlockSpec(memory_space=pltpu.VMEM)] * 3,
        compiler_params=pltpu.CompilerParams(vmem_limit_bytes=8 * 1024 * 1024),
    )(*results)


def solution(mesh):
    return jax.shard_map(
        shards,
        mesh=mesh,
        in_specs=(
            P(None, "dp", "tensor"),
            P(None, "dp", "tensor"),
            P("tensor", None),
            P(None, "dp", "tensor"),
            P(None, "dp", "tensor"),
            P(None, "dp", "tensor"),
        ),
        out_specs=(P("tensor", "dp"), P("dp", "tensor"), P("dp", "tensor")),
        check_vma=False,
    )
```

```python
import jax
import jax.numpy as jnp
from jax import lax
from jax.experimental import pallas as pl
from jax.experimental.pallas import tpu as pltpu
from jax.sharding import PartitionSpec as P

SLOPE_LEVELS = (-0.09, 0.06, 0.22, 0.41, 0.6, 0.79, 0.96, 1.08)
MESH = pl.DeviceIdType.MESH
ROWS = 160
HALF = 80
BLOCK = 256
HIDDEN = 1024
WIDTH = 4096
CHUNKS = 4
DOWN = 2
PIECES = DOWN + CHUNKS
PART = HIDDEN // CHUNKS
WIDE = 2 * PART
N_SENDS = 48
N_SLOTS = 88


def wrap(value):
    return lax.rem(value + 4, 4)


def kernel(
    dy_hbm, x_hbm, w_hbm, s_hbm, u_hbm, code_hbm,
    down_hbm, gate_hbm, up_hbm,
    wv, sv, uv, cv, rows, xz, xt, dyt, relays, gu, h, slopes, xtt, dytt, psend, precv, pown,
    down_ref, gate_ref, up_ref, lsem, osem, ssem, rsem,
):
    dp = lax.axis_index("dp")
    tensor = lax.axis_index("tensor")
    x, zl, c = dp // 4, lax.rem(dp // 2, 2), lax.rem(dp, 2)
    zh, y = tensor // 4, lax.rem(tensor, 4)

    def device(x=x, zl=zl, c=c, zh=zh, y=y):
        return {"dp": x * 4 + zl * 2 + c, "tensor": zh * 4 + y}

    ring = {
        "x+": device(x=wrap(x + 1)), "x-": device(x=wrap(x - 1)),
        "y+": device(y=wrap(y + 1)), "y-": device(y=wrap(y - 1)),
        "z+": device(zh=wrap(zh + 1)), "z-": device(zh=wrap(zh - 1)),
        "core": device(c=1 - c), "pair": device(zl=1 - zl),
    }

    barrier = pltpu.get_barrier_semaphore()
    for peer in ring.values():
        pl.semaphore_signal(barrier, inc=1, device_id=peer, device_id_type=MESH)

    def rows_at(buffer, row, start=0, size=ROWS):
        return buffer.at[pl.ds(pl.multiple_of(row * ROWS + start, 16), size)]

    def at_rows(zh, y, start=0, size=ROWS):
        return rows_at(rows, zh * 4 + y, start, size)

    def at_xz(zh, y, start=0, size=ROWS):
        return rows_at(xz, zh, start, size)

    local = [
        pltpu.make_async_copy(src, dst, lsem.at[i])
        for i, (src, dst) in enumerate((
            (dy_hbm, at_rows(zh, y)), (x_hbm, at_xz(zh, y)), (s_hbm, sv), (u_hbm, uv), (code_hbm, cv), (w_hbm, wv)
        ))
    ]
    for copy in local:
        copy.start()

    sent = []

    slots = []

    def slot():
        slots.append(len(slots))
        return slots[-1]

    def send(src, dst, peer, into=None):
        i = len(sent)
        if i >= N_SENDS:
            sent[i - N_SENDS].wait_send()
        copy = pltpu.make_async_remote_copy(
            src_ref=src, dst_ref=dst, send_sem=ssem.at[i % N_SENDS], recv_sem=rsem.at[slot() if into is None else into],
            device_id=ring[peer], device_id_type=MESH,
        )
        copy.start()
        sent.append(copy)
        return copy

    def landed(block, into):
        pltpu.make_async_remote_copy(
            src_ref=block, dst_ref=block, send_sem=ssem.at[0], recv_sem=rsem.at[into],
            device_id=ring["core"], device_id_type=MESH,
        ).wait_recv()

    class Ring:
        def __init__(self, at, me, axis, split=False):
            self.at, self.me, self.up, self.down, self.split = at, me, axis + "+", axis + "-", split
            self.far = slot()

        def begin(self):
            if self.split:
                top, bottom = self.at(self.me, 0, HALF), self.at(self.me, HALF, HALF)
                self.right = send(top, top, self.up)
                self.left = send(bottom, bottom, self.down)
                self.rest = (send(bottom, bottom, self.up), send(top, top, self.down))
            else:
                block = self.at(self.me)
                self.right = send(block, block, self.up)
                self.left = send(block, block, self.down)
                self.rest = ()

        def take(self):
            self.right.wait_recv()
            half = self.at(wrap(self.me - 1), 0, HALF)
            send(half, half, self.up, self.far)
            self.left.wait_recv()
            half = self.at(wrap(self.me + 1), HALF, HALF)
            send(half, half, self.down, self.far)
            for copy in self.rest:
                copy.wait_recv()

        def take_far(self):
            landed(self.at(wrap(self.me + 2)), self.far)

    class Turn:
        def __init__(self, source, buffer, i):
            self.source, self.buffer, self.relay, self.i = source, buffer, relays.at[i], i
            self.origin = (x, wrap(x - 1), wrap(x + 1), wrap(x + 2))
            self.far, self.core = slot(), slot()
            self.over_y = [
                Ring(lambda yo, start=0, size=ROWS, o=o: self.at(yo, o, start, size), y, "y") for o in self.origin
            ]

        def at(self, yo, xo, start=0, size=ROWS):
            return rows_at(self.buffer, yo * 8 + c * 4 + xo, start, size)

        def begin(self):
            self.kept = pltpu.make_async_copy(self.source(x), self.at(y, x), lsem.at[6 + self.i])
            self.kept.start()
            self.far_top = send(self.source(wrap(x + 2), 0, HALF), self.relay.at[0], "x+")
            self.far_bottom = send(self.source(wrap(x + 2), HALF, HALF), self.relay.at[1], "x-")
            self.right = send(self.source(wrap(x + 1)), self.at(y, x), "x+")
            self.left = send(self.source(wrap(x - 1)), self.at(y, x), "x-")

        def pass_on(self):
            self.far_top.wait_recv()
            send(self.relay.at[0], self.at(y, wrap(x - 1), 0, HALF), "x+", self.far)
            self.far_bottom.wait_recv()
            send(self.relay.at[1], self.at(y, wrap(x + 1), HALF, HALF), "x-", self.far)

        def along_y(self, b):
            if b == 0:
                self.kept.wait()
            elif b == 1:
                self.right.wait_recv()
            elif b == 2:
                self.left.wait_recv()
            else:
                landed(self.at(y, wrap(x + 2)), self.far)
            self.over_y[b].begin()

        def arrive(self, b):
            self.over_y[b].take_far()
            for yo in (1 - c, 3 - c):
                block = self.at(yo, self.origin[b])
                send(block, block, "core", self.core)

        def finish(self):
            landed(self.buffer.at[pl.ds(pl.multiple_of(c * (8 * ROWS), 16), 8 * ROWS)], self.core)

        def turn(self, out):
            for i in range(2):
                for r in range(5):
                    start = pl.multiple_of((2 * i + c) * (8 * ROWS) + r * 256, 256)
                    out[i, :, r * 256 : (r + 1) * 256] = self.buffer[pl.ds(start, 256), :].T

    class Piece:
        def __init__(self, k):
            self.k = k
            self.over_x = Ring(self.at(k), x, "x")
            self.core = slot()

        def at(self, k):
            return lambda xo, start=0, size=ROWS: rows_at(gu.at[k], c * 4 + xo, start, size)

        def share(self, origin):
            block = self.over_x.at(origin)
            send(block, block, "core", self.core)

        def begin(self):
            self.over_x.begin()
            self.share(x)

        def take(self):
            self.over_x.take()
            self.share(wrap(x - 1))
            self.share(wrap(x + 1))

        def take_far(self):
            self.over_x.take_far()
            self.share(wrap(x + 2))

        def finish(self):
            landed(gu.at[self.k].at[pl.ds(pl.multiple_of((1 - c) * (4 * ROWS), 16), 4 * ROWS)], self.core)

    own_rows = pl.ds(pl.multiple_of((c * 4 + x) * ROWS, 16), ROWS)
    local[2].wait()
    local[3].wait()
    for k in range(DOWN):
        columns = slice(k * WIDE, (k + 1) * WIDE)
        gu[k, own_rows, :] = (sv[:, columns].astype(jnp.float32) * uv[:, columns].astype(jnp.float32)).astype(jnp.bfloat16)
    local[0].wait()
    local[1].wait()
    pl.semaphore_wait(barrier, len(ring))

    origins = (zh, wrap(zh - 1), wrap(zh + 1), wrap(zh + 2))
    rows_z = Ring(lambda zo, start=0, size=ROWS: at_rows(zo, y, start, size), zh, "z", True)
    rows_y = [Ring(lambda yo, start=0, size=ROWS, o=o: at_rows(o, yo, start, size), y, "y") for o in origins]
    x_z = Ring(lambda zo, start=0, size=ROWS: at_xz(zo, y, start, size), zh, "z", True)
    turn_d = Turn(lambda zo, start=0, size=ROWS: at_rows(zo, y, start, size), dyt, 0)
    turn_x = Turn(lambda zo, start=0, size=ROWS: at_xz(zo, y, start, size), xt, 1)
    pieces = [Piece(k) for k in range(PIECES)]

    rows_z.begin()
    rows_y[0].begin()
    pieces[0].begin()
    pieces[1].begin()

    local[4].wait()
    token = lax.broadcasted_iota(jnp.int32, (HALF, HALF), 0)
    place = lax.broadcasted_iota(jnp.int32, (HALF, HALF), 1)
    order = (place == lax.rem(token, 10) * 8 + token // 10).astype(jnp.float32).astype(jnp.bfloat16)
    for m in range(2):
        words = cv[m * 8 : m * 8 + 8, :]
        codes = jnp.concatenate(
            [jnp.bitwise_and(jnp.right_shift(words, 3 * k), 7).astype(jnp.float32) for k in range(10)], axis=0
        ).astype(jnp.bfloat16)
        codes = jnp.dot(order, codes, preferred_element_type=jnp.float32)
        level = jnp.full(codes.shape, SLOPE_LEVELS[0], jnp.float32)
        for symbol in range(1, 8):
            level = jnp.where(codes == jnp.float32(symbol), jnp.float32(SLOPE_LEVELS[symbol]), level)
        slopes[m * HALF : m * HALF + HALF, :] = level
    local[5].wait()

    def multiply(b, yo, first=False):
        z = origins[b]
        weights = wv[:, pl.ds(pl.multiple_of((z * 4 + yo) * BLOCK, BLOCK), BLOCK)]
        product = lax.dot_general(
            at_rows(z, yo)[...], weights, (((1,), (1,)), ((), ())), preferred_element_type=jnp.float32
        )
        h[...] = product if first else h[...] + product

    def activations(k):
        columns = slice(k * PART, (k + 1) * PART)
        grad = h[:, columns]
        gate = grad * uv[:, columns].astype(jnp.float32) * slopes[:, columns]
        gu[DOWN + k, own_rows, 0:PART] = gate.astype(jnp.bfloat16)
        gu[DOWN + k, own_rows, PART:WIDE] = (grad * sv[:, columns].astype(jnp.float32)).astype(jnp.bfloat16)

    partials = {}
    outward = []

    def products(k):
        pieces[k].finish()
        lhs = dytt if k < DOWN else xtt
        values = gu[k]
        psend[k] = jnp.dot(lhs[1 - zl], values, preferred_element_type=jnp.float32).astype(jnp.bfloat16)
        partials[k] = send(psend.at[k], precv.at[k], "pair")
        pown[k] = jnp.dot(lhs[zl], values, preferred_element_type=jnp.float32)

    def put(src, dst):
        copy = pltpu.make_async_copy(src, dst, osem.at[len(outward)])
        copy.start()
        outward.append(copy)

    def total(k):
        partials[k].wait_recv()
        whole = pown[k] + precv[k].astype(jnp.float32)
        if k < DOWN:
            part = slice(k * WIDE, (k + 1) * WIDE)
            down_ref[part, :] = whole.T.astype(jnp.bfloat16)
            put(down_ref.at[part], down_hbm.at[part])
        else:
            part = slice((k - DOWN) * PART, (k - DOWN + 1) * PART)
            gate_ref[:, part] = whole[:, 0:PART].astype(jnp.bfloat16)
            put(gate_ref.at[:, part], gate_hbm.at[:, part])
            up_ref[:, part] = whole[:, PART:WIDE].astype(jnp.bfloat16)
            put(up_ref.at[:, part], up_hbm.at[:, part])

    multiply(0, y, True)
    rows_z.take()
    rows_y[1].begin()
    rows_y[2].begin()
    x_z.begin()
    rows_y[0].take()
    multiply(1, y)
    multiply(2, y)
    rows_z.take_far()
    turn_d.begin()
    rows_y[3].begin()
    turn_d.along_y(0)
    multiply(3, y)
    multiply(0, wrap(y - 1))
    multiply(0, wrap(y + 1))
    rows_y[1].take()
    multiply(1, wrap(y - 1))
    multiply(1, wrap(y + 1))
    rows_y[2].take()
    turn_d.pass_on()
    turn_d.along_y(1)
    turn_d.along_y(2)
    x_z.take()
    rows_y[3].take()
    multiply(2, wrap(y - 1))
    multiply(2, wrap(y + 1))
    turn_d.along_y(3)
    turn_d.over_y[0].take()
    pieces[0].take()
    x_z.take_far()
    turn_x.begin()
    multiply(3, wrap(y - 1))
    multiply(3, wrap(y + 1))
    for b in range(3):
        rows_y[b].take_far()
        multiply(b, wrap(y + 2))
    turn_d.over_y[1].take()
    turn_d.over_y[2].take()
    pieces[1].take()
    turn_d.arrive(0)
    rows_y[3].take_far()
    multiply(3, wrap(y + 2))
    turn_x.pass_on()
    activations(0)
    pieces[2].begin()
    turn_d.over_y[3].take()
    activations(1)
    pieces[3].begin()
    turn_x.along_y(0)
    turn_x.along_y(1)
    pieces[0].take_far()
    turn_x.along_y(2)
    turn_d.arrive(1)
    turn_d.arrive(2)
    activations(2)
    activations(3)
    pieces[1].take_far()
    turn_d.arrive(3)
    turn_d.finish()
    turn_d.turn(dytt)
    products(0)
    turn_x.over_y[0].take()
    turn_x.along_y(3)
    pieces[2].take()
    products(1)
    pieces[4].begin()
    turn_x.over_y[1].take()
    turn_x.over_y[2].take()
    pieces[3].take()
    turn_x.over_y[3].take()
    turn_x.arrive(0)
    pieces[2].take_far()
    pieces[5].begin()
    turn_x.arrive(1)
    turn_x.arrive(2)
    pieces[4].take()
    turn_x.arrive(3)
    turn_x.finish()
    turn_x.turn(xtt)
    products(2)
    pieces[3].take_far()
    pieces[5].take()
    products(3)
    pieces[4].take_far()
    products(4)
    total(0)
    total(1)
    pieces[5].take_far()
    products(5)
    for k in range(DOWN, PIECES):
        total(k)
    assert len(slots) <= N_SLOTS
    for copy in outward:
        copy.wait()
    for copy in sent[-N_SENDS:]:
        copy.wait_send()


def hand_over(*refs):
    for src, dst in zip(refs[:3], refs[3:]):
        dst[...] = src[...]


def shards(out_grad, layer_input, w_down, silu_gate, up_proj, slope_codes):
    bf16, f32 = jnp.bfloat16, jnp.float32
    vmem = pltpu.VMEM
    anywhere = pl.BlockSpec(memory_space=pl.ANY)
    results = pl.pallas_call(
        kernel,
        out_shape=(
            jax.ShapeDtypeStruct((HIDDEN, BLOCK), bf16),
            jax.ShapeDtypeStruct((BLOCK, HIDDEN), bf16),
            jax.ShapeDtypeStruct((BLOCK, HIDDEN), bf16),
        ),
        in_specs=[pl.BlockSpec(memory_space=pltpu.HBM)] * 6,
        out_specs=[anywhere] * 3,
        scratch_shapes=[
            vmem((HIDDEN, WIDTH), bf16),
            vmem((ROWS, HIDDEN), bf16),
            vmem((ROWS, HIDDEN), bf16),
            vmem((16, HIDDEN), jnp.int32),
            vmem((16 * ROWS, BLOCK), bf16),
            vmem((4 * ROWS, BLOCK), bf16),
            vmem((32 * ROWS, BLOCK), bf16),
            vmem((32 * ROWS, BLOCK), bf16),
            vmem((2, 2, HALF, BLOCK), bf16),
            vmem((PIECES, 8 * ROWS, WIDE), bf16),
            vmem((ROWS, HIDDEN), f32),
            vmem((ROWS, HIDDEN), f32),
            vmem((2, BLOCK, 8 * ROWS), bf16),
            vmem((2, BLOCK, 8 * ROWS), bf16),
            vmem((PIECES, BLOCK, WIDE), bf16),
            vmem((PIECES, BLOCK, WIDE), bf16),
            vmem((PIECES, BLOCK, WIDE), f32),
            vmem((HIDDEN, BLOCK), bf16),
            vmem((BLOCK, HIDDEN), bf16),
            vmem((BLOCK, HIDDEN), bf16),
            pltpu.SemaphoreType.DMA((8,)),
            pltpu.SemaphoreType.DMA((2 * CHUNKS + DOWN,)),
            pltpu.SemaphoreType.DMA((N_SENDS,)),
            pltpu.SemaphoreType.DMA((N_SLOTS,)),
        ],
        compiler_params=pltpu.CompilerParams(
            collective_id=0, has_side_effects=True, vmem_limit_bytes=44 * 1024 * 1024
        ),
    )(
        *(
            pltpu.with_memory_space_constraint(a, pltpu.HBM)
            for a in (
                out_grad.reshape(ROWS, BLOCK),
                layer_input.reshape(ROWS, BLOCK),
                w_down,
                silu_gate.reshape(ROWS, HIDDEN),
                up_proj.reshape(ROWS, HIDDEN),
                slope_codes.reshape(16, HIDDEN),
            )
        )
    )
    return pl.pallas_call(
        hand_over,
        out_shape=tuple(jax.ShapeDtypeStruct(a.shape, a.dtype) for a in results),
        in_specs=[pl.BlockSpec(memory_space=pltpu.VMEM)] * 3,
        out_specs=[pl.BlockSpec(memory_space=pltpu.VMEM)] * 3,
        compiler_params=pltpu.CompilerParams(vmem_limit_bytes=8 * 1024 * 1024),
    )(*results)


def solution(mesh):
    return jax.shard_map(
        shards,
        mesh=mesh,
        in_specs=(
            P(None, "dp", "tensor"),
            P(None, "dp", "tensor"),
            P("tensor", None),
            P(None, "dp", "tensor"),
            P(None, "dp", "tensor"),
            P(None, "dp", "tensor"),
        ),
        out_specs=(P("tensor", "dp"), P("dp", "tensor"), P("dp", "tensor")),
        check_vma=False,
    )
```

```python
import jax
import jax.numpy as jnp
from jax import lax
from jax.experimental import pallas as pl
from jax.experimental.pallas import tpu as pltpu
from jax.sharding import PartitionSpec as P

SLOPE_LEVELS = (-0.09, 0.06, 0.22, 0.41, 0.6, 0.79, 0.96, 1.08)
MESH = pl.DeviceIdType.MESH
ROWS = 160
HALF = 80
BLOCK = 256
HIDDEN = 1024
WIDTH = 4096
CHUNKS = 4
DOWN = 2
PIECES = DOWN + CHUNKS
PART = HIDDEN // CHUNKS
WIDE = 2 * PART
N_SENDS = 48
N_SLOTS = 88


def wrap(value):
    return lax.rem(value + 4, 4)


def kernel(
    dy_hbm, x_hbm, w_hbm, s_hbm, u_hbm, code_hbm,
    down_hbm, gate_hbm, up_hbm,
    wv, sv, uv, cv, rows, xz, xt, dyt, relays, gu, h, slopes, xtt, dytt, psend, precv, pown,
    down_ref, gate_ref, up_ref, lsem, osem, ssem, rsem,
):
    dp = lax.axis_index("dp")
    tensor = lax.axis_index("tensor")
    x, zl, c = dp // 4, lax.rem(dp // 2, 2), lax.rem(dp, 2)
    zh, y = tensor // 4, lax.rem(tensor, 4)

    def device(x=x, zl=zl, c=c, zh=zh, y=y):
        return {"dp": x * 4 + zl * 2 + c, "tensor": zh * 4 + y}

    ring = {
        "x+": device(x=wrap(x + 1)), "x-": device(x=wrap(x - 1)),
        "y+": device(y=wrap(y + 1)), "y-": device(y=wrap(y - 1)),
        "z+": device(zh=wrap(zh + 1)), "z-": device(zh=wrap(zh - 1)),
        "core": device(c=1 - c), "pair": device(zl=1 - zl),
    }

    barrier = pltpu.get_barrier_semaphore()
    for peer in ring.values():
        pl.semaphore_signal(barrier, inc=1, device_id=peer, device_id_type=MESH)

    def rows_at(buffer, row, start=0, size=ROWS):
        return buffer.at[pl.ds(pl.multiple_of(row * ROWS + start, 16), size)]

    def at_rows(zh, y, start=0, size=ROWS):
        return rows_at(rows, zh * 4 + y, start, size)

    def at_xz(zh, y, start=0, size=ROWS):
        return rows_at(xz, zh, start, size)

    local = [
        pltpu.make_async_copy(src, dst, lsem.at[i])
        for i, (src, dst) in enumerate((
            (dy_hbm, at_rows(zh, y)), (x_hbm, at_xz(zh, y)), (s_hbm, sv), (u_hbm, uv), (code_hbm, cv), (w_hbm, wv)
        ))
    ]
    for copy in local:
        copy.start()

    sent = []

    slots = []

    def slot():
        slots.append(len(slots))
        return slots[-1]

    def send(src, dst, peer, into=None):
        i = len(sent)
        if i >= N_SENDS:
            sent[i - N_SENDS].wait_send()
        copy = pltpu.make_async_remote_copy(
            src_ref=src, dst_ref=dst, send_sem=ssem.at[i % N_SENDS], recv_sem=rsem.at[slot() if into is None else into],
            device_id=ring[peer], device_id_type=MESH,
        )
        copy.start()
        sent.append(copy)
        return copy

    def landed(block, into):
        pltpu.make_async_remote_copy(
            src_ref=block, dst_ref=block, send_sem=ssem.at[0], recv_sem=rsem.at[into],
            device_id=ring["core"], device_id_type=MESH,
        ).wait_recv()

    class Ring:
        def __init__(self, at, me, axis, split=False):
            self.at, self.me, self.up, self.down, self.split = at, me, axis + "+", axis + "-", split
            self.far = slot()

        def begin(self):
            if self.split:
                top, bottom = self.at(self.me, 0, HALF), self.at(self.me, HALF, HALF)
                self.right = send(top, top, self.up)
                self.left = send(bottom, bottom, self.down)
                self.rest = (send(bottom, bottom, self.up), send(top, top, self.down))
            else:
                block = self.at(self.me)
                self.right = send(block, block, self.up)
                self.left = send(block, block, self.down)
                self.rest = ()

        def take(self):
            self.right.wait_recv()
            half = self.at(wrap(self.me - 1), 0, HALF)
            send(half, half, self.up, self.far)
            self.left.wait_recv()
            half = self.at(wrap(self.me + 1), HALF, HALF)
            send(half, half, self.down, self.far)
            for copy in self.rest:
                copy.wait_recv()

        def take_far(self):
            landed(self.at(wrap(self.me + 2)), self.far)

    class Turn:
        def __init__(self, source, buffer, i):
            self.source, self.buffer, self.relay, self.i = source, buffer, relays.at[i], i
            self.origin = (x, wrap(x - 1), wrap(x + 1), wrap(x + 2))
            self.far, self.core = slot(), slot()
            self.over_y = [
                Ring(lambda yo, start=0, size=ROWS, o=o: self.at(yo, o, start, size), y, "y") for o in self.origin
            ]

        def at(self, yo, xo, start=0, size=ROWS):
            return rows_at(self.buffer, yo * 8 + c * 4 + xo, start, size)

        def begin(self):
            self.kept = pltpu.make_async_copy(self.source(x), self.at(y, x), lsem.at[6 + self.i])
            self.kept.start()
            self.far_top = send(self.source(wrap(x + 2), 0, HALF), self.relay.at[0], "x+")
            self.far_bottom = send(self.source(wrap(x + 2), HALF, HALF), self.relay.at[1], "x-")
            self.right = send(self.source(wrap(x + 1)), self.at(y, x), "x+")
            self.left = send(self.source(wrap(x - 1)), self.at(y, x), "x-")

        def pass_on(self):
            self.far_top.wait_recv()
            send(self.relay.at[0], self.at(y, wrap(x - 1), 0, HALF), "x+", self.far)
            self.far_bottom.wait_recv()
            send(self.relay.at[1], self.at(y, wrap(x + 1), HALF, HALF), "x-", self.far)

        def along_y(self, b):
            if b == 0:
                self.kept.wait()
            elif b == 1:
                self.right.wait_recv()
            elif b == 2:
                self.left.wait_recv()
            else:
                landed(self.at(y, wrap(x + 2)), self.far)
            self.over_y[b].begin()

        def arrive(self, b):
            self.over_y[b].take_far()
            for yo in (1 - c, 3 - c):
                block = self.at(yo, self.origin[b])
                send(block, block, "core", self.core)

        def finish(self):
            landed(self.buffer.at[pl.ds(pl.multiple_of(c * (8 * ROWS), 16), 8 * ROWS)], self.core)

        def turn(self, out):
            for i in range(2):
                for r in range(5):
                    start = pl.multiple_of((2 * i + c) * (8 * ROWS) + r * 256, 256)
                    out[i, :, r * 256 : (r + 1) * 256] = self.buffer[pl.ds(start, 256), :].T

    class Piece:
        def __init__(self, k):
            self.k = k
            self.over_x = Ring(self.at(k), x, "x")
            self.core = slot()

        def at(self, k):
            return lambda xo, start=0, size=ROWS: rows_at(gu.at[k], c * 4 + xo, start, size)

        def share(self, origin):
            block = self.over_x.at(origin)
            send(block, block, "core", self.core)

        def begin(self):
            self.over_x.begin()
            self.share(x)

        def take(self):
            self.over_x.take()
            self.share(wrap(x - 1))
            self.share(wrap(x + 1))

        def take_far(self):
            self.over_x.take_far()
            self.share(wrap(x + 2))

        def finish(self):
            landed(gu.at[self.k].at[pl.ds(pl.multiple_of((1 - c) * (4 * ROWS), 16), 4 * ROWS)], self.core)

    own_rows = pl.ds(pl.multiple_of((c * 4 + x) * ROWS, 16), ROWS)
    local[2].wait()
    local[3].wait()
    for k in range(DOWN):
        columns = slice(k * WIDE, (k + 1) * WIDE)
        gu[k, own_rows, :] = (sv[:, columns].astype(jnp.float32) * uv[:, columns].astype(jnp.float32)).astype(jnp.bfloat16)
    local[0].wait()
    local[1].wait()
    pl.semaphore_wait(barrier, len(ring))

    origins = (zh, wrap(zh - 1), wrap(zh + 1), wrap(zh + 2))
    rows_z = Ring(lambda zo, start=0, size=ROWS: at_rows(zo, y, start, size), zh, "z", True)
    rows_y = [Ring(lambda yo, start=0, size=ROWS, o=o: at_rows(o, yo, start, size), y, "y") for o in origins]
    x_z = Ring(lambda zo, start=0, size=ROWS: at_xz(zo, y, start, size), zh, "z", True)
    turn_d = Turn(lambda zo, start=0, size=ROWS: at_rows(zo, y, start, size), dyt, 0)
    turn_x = Turn(lambda zo, start=0, size=ROWS: at_xz(zo, y, start, size), xt, 1)
    pieces = [Piece(k) for k in range(PIECES)]

    rows_z.begin()
    rows_y[0].begin()
    pieces[0].begin()
    pieces[1].begin()

    local[4].wait()
    token = lax.broadcasted_iota(jnp.int32, (HALF, HALF), 0)
    place = lax.broadcasted_iota(jnp.int32, (HALF, HALF), 1)
    order = (place == lax.rem(token, 10) * 8 + token // 10).astype(jnp.float32).astype(jnp.bfloat16)
    for m in range(2):
        words = cv[m * 8 : m * 8 + 8, :]
        codes = jnp.concatenate(
            [jnp.bitwise_and(jnp.right_shift(words, 3 * k), 7).astype(jnp.float32) for k in range(10)], axis=0
        ).astype(jnp.bfloat16)
        codes = jnp.dot(order, codes, preferred_element_type=jnp.float32)
        level = jnp.full(codes.shape, SLOPE_LEVELS[0], jnp.float32)
        for symbol in range(1, 8):
            level = jnp.where(codes == jnp.float32(symbol), jnp.float32(SLOPE_LEVELS[symbol]), level)
        slopes[m * HALF : m * HALF + HALF, :] = level
    local[5].wait()

    def multiply(b, yo, first=False):
        z = origins[b]
        weights = wv[:, pl.ds(pl.multiple_of((z * 4 + yo) * BLOCK, BLOCK), BLOCK)]
        product = lax.dot_general(
            at_rows(z, yo)[...], weights, (((1,), (1,)), ((), ())), preferred_element_type=jnp.float32
        )
        h[...] = product if first else h[...] + product

    def activations(k):
        columns = slice(k * PART, (k + 1) * PART)
        grad = h[:, columns]
        gate = grad * uv[:, columns].astype(jnp.float32) * slopes[:, columns]
        gu[DOWN + k, own_rows, 0:PART] = gate.astype(jnp.bfloat16)
        gu[DOWN + k, own_rows, PART:WIDE] = (grad * sv[:, columns].astype(jnp.float32)).astype(jnp.bfloat16)

    partials = {}
    outward = []

    def products(k):
        pieces[k].finish()
        lhs = dytt if k < DOWN else xtt
        values = gu[k]
        psend[k] = jnp.dot(lhs[1 - zl], values, preferred_element_type=jnp.float32).astype(jnp.bfloat16)
        partials[k] = send(psend.at[k], precv.at[k], "pair")
        pown[k] = jnp.dot(lhs[zl], values, preferred_element_type=jnp.float32)

    def put(src, dst):
        copy = pltpu.make_async_copy(src, dst, osem.at[len(outward)])
        copy.start()
        outward.append(copy)

    def total(k):
        partials[k].wait_recv()
        whole = pown[k] + precv[k].astype(jnp.float32)
        if k < DOWN:
            part = slice(k * WIDE, (k + 1) * WIDE)
            down_ref[part, :] = whole.T.astype(jnp.bfloat16)
            put(down_ref.at[part], down_hbm.at[part])
        else:
            part = slice((k - DOWN) * PART, (k - DOWN + 1) * PART)
            gate_ref[:, part] = whole[:, 0:PART].astype(jnp.bfloat16)
            put(gate_ref.at[:, part], gate_hbm.at[:, part])
            up_ref[:, part] = whole[:, PART:WIDE].astype(jnp.bfloat16)
            put(up_ref.at[:, part], up_hbm.at[:, part])

    multiply(0, y, True)
    rows_z.take()
    rows_y[1].begin()
    rows_y[2].begin()
    x_z.begin()
    rows_y[0].take()
    multiply(1, y)
    multiply(2, y)
    rows_z.take_far()
    turn_d.begin()
    rows_y[3].begin()
    turn_d.along_y(0)
    multiply(3, y)
    multiply(0, wrap(y - 1))
    multiply(0, wrap(y + 1))
    rows_y[1].take()
    turn_d.pass_on()
    rows_y[2].take()
    turn_d.along_y(1)
    turn_d.along_y(2)
    x_z.take()
    turn_d.along_y(3)
    rows_y[3].take()
    turn_d.over_y[0].take()
    multiply(1, wrap(y - 1))
    multiply(1, wrap(y + 1))
    multiply(2, wrap(y - 1))
    multiply(2, wrap(y + 1))
    pieces[0].take()
    pieces[1].take()
    x_z.take_far()
    turn_x.begin()
    turn_d.over_y[1].take()
    turn_d.over_y[2].take()
    multiply(3, wrap(y - 1))
    multiply(3, wrap(y + 1))
    for b in range(3):
        rows_y[b].take_far()
        multiply(b, wrap(y + 2))
    turn_d.over_y[3].take()
    turn_x.pass_on()
    rows_y[3].take_far()
    multiply(3, wrap(y + 2))
    activations(0)
    pieces[2].begin()
    turn_d.arrive(0)
    activations(1)
    pieces[3].begin()
    turn_x.along_y(0)
    turn_x.along_y(1)
    pieces[0].take_far()
    turn_x.along_y(2)
    turn_d.arrive(1)
    turn_d.arrive(2)
    turn_d.arrive(3)
    turn_d.finish()
    turn_d.turn(dytt)
    products(0)
    pieces[1].take_far()
    activations(2)
    activations(3)
    turn_x.over_y[0].take()
    turn_x.along_y(3)
    pieces[2].take()
    products(1)
    pieces[4].begin()
    turn_x.over_y[1].take()
    turn_x.over_y[2].take()
    pieces[3].take()
    turn_x.over_y[3].take()
    turn_x.arrive(0)
    pieces[2].take_far()
    pieces[5].begin()
    turn_x.arrive(1)
    turn_x.arrive(2)
    pieces[4].take()
    turn_x.arrive(3)
    turn_x.finish()
    turn_x.turn(xtt)
    products(2)
    pieces[3].take_far()
    pieces[5].take()
    products(3)
    pieces[4].take_far()
    products(4)
    total(0)
    total(1)
    pieces[5].take_far()
    products(5)
    for k in range(DOWN, PIECES):
        total(k)
    assert len(slots) <= N_SLOTS
    for copy in outward:
        copy.wait()
    for copy in sent[-N_SENDS:]:
        copy.wait_send()


def hand_over(*refs):
    for src, dst in zip(refs[:3], refs[3:]):
        dst[...] = src[...]


def shards(out_grad, layer_input, w_down, silu_gate, up_proj, slope_codes):
    bf16, f32 = jnp.bfloat16, jnp.float32
    vmem = pltpu.VMEM
    anywhere = pl.BlockSpec(memory_space=pl.ANY)
    results = pl.pallas_call(
        kernel,
        out_shape=(
            jax.ShapeDtypeStruct((HIDDEN, BLOCK), bf16),
            jax.ShapeDtypeStruct((BLOCK, HIDDEN), bf16),
            jax.ShapeDtypeStruct((BLOCK, HIDDEN), bf16),
        ),
        in_specs=[pl.BlockSpec(memory_space=pltpu.HBM)] * 6,
        out_specs=[anywhere] * 3,
        scratch_shapes=[
            vmem((HIDDEN, WIDTH), bf16),
            vmem((ROWS, HIDDEN), bf16),
            vmem((ROWS, HIDDEN), bf16),
            vmem((16, HIDDEN), jnp.int32),
            vmem((16 * ROWS, BLOCK), bf16),
            vmem((4 * ROWS, BLOCK), bf16),
            vmem((32 * ROWS, BLOCK), bf16),
            vmem((32 * ROWS, BLOCK), bf16),
            vmem((2, 2, HALF, BLOCK), bf16),
            vmem((PIECES, 8 * ROWS, WIDE), bf16),
            vmem((ROWS, HIDDEN), f32),
            vmem((ROWS, HIDDEN), f32),
            vmem((2, BLOCK, 8 * ROWS), bf16),
            vmem((2, BLOCK, 8 * ROWS), bf16),
            vmem((PIECES, BLOCK, WIDE), bf16),
            vmem((PIECES, BLOCK, WIDE), bf16),
            vmem((PIECES, BLOCK, WIDE), f32),
            vmem((HIDDEN, BLOCK), bf16),
            vmem((BLOCK, HIDDEN), bf16),
            vmem((BLOCK, HIDDEN), bf16),
            pltpu.SemaphoreType.DMA((8,)),
            pltpu.SemaphoreType.DMA((2 * CHUNKS + DOWN,)),
            pltpu.SemaphoreType.DMA((N_SENDS,)),
            pltpu.SemaphoreType.DMA((N_SLOTS,)),
        ],
        compiler_params=pltpu.CompilerParams(
            collective_id=0, has_side_effects=True, vmem_limit_bytes=44 * 1024 * 1024
        ),
    )(
        *(
            pltpu.with_memory_space_constraint(a, pltpu.HBM)
            for a in (
                out_grad.reshape(ROWS, BLOCK),
                layer_input.reshape(ROWS, BLOCK),
                w_down,
                silu_gate.reshape(ROWS, HIDDEN),
                up_proj.reshape(ROWS, HIDDEN),
                slope_codes.reshape(16, HIDDEN),
            )
        )
    )
    return pl.pallas_call(
        hand_over,
        out_shape=tuple(jax.ShapeDtypeStruct(a.shape, a.dtype) for a in results),
        in_specs=[pl.BlockSpec(memory_space=pltpu.VMEM)] * 3,
        out_specs=[pl.BlockSpec(memory_space=pltpu.VMEM)] * 3,
        compiler_params=pltpu.CompilerParams(vmem_limit_bytes=8 * 1024 * 1024),
    )(*results)


def solution(mesh):
    return jax.shard_map(
        shards,
        mesh=mesh,
        in_specs=(
            P(None, "dp", "tensor"),
            P(None, "dp", "tensor"),
            P("tensor", None),
            P(None, "dp", "tensor"),
            P(None, "dp", "tensor"),
            P(None, "dp", "tensor"),
        ),
        out_specs=(P("tensor", "dp"), P("dp", "tensor"), P("dp", "tensor")),
        check_vma=False,
    )
```
